32 devices in a mesh: pts: 16 (over z, y, x), rows: 2 (over core).
Axes of the slice: x: 2, y: 2, z: 4, core: 2. Of those that a mesh axis runs over, the one named last changes fastest.
Arguments:
- vertex: bfloat16 [16, 960, 960], P('pts', 'rows'), may hold values from -0.1875 to 0.1875
- bubble: float32 [16, 960], P('pts'), may hold values from -2 to -0.2
- cross_deriv: bfloat16 [16, 960, 960], P('pts', 'rows'), may hold values from -6 to 6
- send_blocks: int32 [16, 16, 2], P('pts'), may hold values from -1 to 14, as said below
- recv_slots: int32 [16, 15], P('pts'), may hold values from 0 to 31, as said below
- freq_shift: int32 [16, 15], P('pts'), may hold values from -16 to 16
- proj_coef: float32 [16, 15], P('pts'), may hold values from -1.5 to 1.5
Outputs:
- left_insertion: bfloat16 [16, 960, 960], P('pts', 'rows')
The draws below stay inside these ranges and needn't reach their ends.
Inputs may be any that keep to these rules, and one draw needn't show every extreme that they name: `send_blocks`: entry [d, e, c] is -1 for an empty slot, else the index p * 15 + g of the box (local point p, form factor g) of device d along pts that fills slot c towards device e. For every e some d fills all 2 slots towards e. `recv_slots`: entry [q, f] is 2 * d + c for a slot c towards device q // 1 along pts whose send_blocks entry [d, q, c] is not -1; each such slot is named by exactly one entry of that device's points.
All inputs are finite; a program needn't handle non-finite values.
Results may differ from the reference program's by a relative error of at most 0.0058.
Values may be sent and summed in bfloat16 or wider, within the bound.
No kernel may reach another device: no remote copies, remote signals or barrier semaphores. Data moves between devices by JAX's collectives and lax.ppermute only.
A program may use at most 128 MiB of HBM per device.

```python
import jax
import jax.numpy as jnp
from jax import lax

NFF = 15
NFREQ = 64
ORDER = 960
PT_DEV = 1
POINTS = 16
CAP = 2
N_PTS = 16


def routing(key):
    possible_targets = N_PTS * CAP
    wanted_count = PT_DEV * NFF
    extra_weight_each_processor = jax.random.randint(jax.random.fold_in(key, 1), (N_PTS,), 0, 3)
    hot_dev = jax.random.randint(jax.random.fold_in(key, 2), (N_PTS,), 0, N_PTS)
    sorted_positions = jax.vmap(lambda k: jax.random.permutation(k, possible_targets))(jax.random.split(jax.random.fold_in(key, 3), N_PTS))
    possible_processor = jnp.arange(possible_targets, dtype=jnp.int32) // CAP
    heavy_marker = (possible_processor[None, :] == hot_dev[:, None]).astype(jnp.int32)
    rating_numbers = sorted_positions.astype(jnp.int32) + possible_targets * (extra_weight_each_processor[possible_processor][None, :] + 3 * heavy_marker)
    unused, chosen = lax.top_k(rating_numbers, wanted_count)
    mixing = jax.vmap(lambda k: jax.random.permutation(k, wanted_count))(jax.random.split(jax.random.fold_in(key, 4), N_PTS))
    chosen = jnp.take_along_axis(chosen, mixing, axis=1).astype(jnp.int32)
    block_ids = jax.random.randint(jax.random.fold_in(key, 5), (N_PTS, wanted_count), 0, wanted_count)
    rows_dest = jnp.broadcast_to(jnp.arange(N_PTS, dtype=jnp.int32)[:, None], (N_PTS, wanted_count))
    table = jnp.full((N_PTS, possible_targets), -1, jnp.int32).at[rows_dest, chosen].set(block_ids.astype(jnp.int32))
    outbound_routing_grid = table.reshape(N_PTS, N_PTS, CAP).transpose(1, 0, 2)
    recv_table = chosen.reshape(N_PTS * PT_DEV, NFF)
    return (outbound_routing_grid, recv_table)


def draw_send_blocks(key, part):
    return routing(jax.random.fold_in(key, 7))[0]


def draw_recv_slots(key, part):
    return routing(jax.random.fold_in(key, 7))[1]


def set_ends(array, stream_key, smallest, top_value):
    longest = array.shape.index(max(array.shape))
    spots = []
    for shift in (0, 1):
        where = [jax.random.randint(jax.random.fold_in(stream_key, axis), (), 0, length) for axis, length in enumerate(array.shape)]
        where[longest] = (where[longest] + shift) % array.shape[longest]
        spots.append(tuple(where))
    return array.at[spots[0]].set(smallest).at[spots[1]].set(top_value)


def block_levels(key, shape, cuts, least, high):
    level, own = 1.0, jax.random.fold_in(key, 6)
    for position, shards_of in cuts:
        draws = jnp.exp(jax.random.uniform(jax.random.fold_in(own, position), (shards_of,), jnp.float32, least / len(cuts), high / len(cuts)))
        level = level * jnp.repeat(draws, shape[position] // shards_of).reshape([-1 if axis == position else 1 for axis in range(len(shape))])
    return level


def gaussian(rng, dims, width, limit, shards=(), kind=jnp.bfloat16):
    loudness = block_levels(rng, dims, shards, -0.22, 0.18) if shards else 1.0
    array = jax.random.normal(rng, dims, jnp.float32) * width * loudness
    return jnp.minimum(jnp.maximum(array, -limit), limit).astype(kind)


def setup_inputs(seed: int = 0) -> dict:
    key_list = jax.random.split(jax.random.key(seed), 8)
    return {
        "vertex": gaussian(key_list[0], (POINTS, ORDER, ORDER), ORDER ** -0.5, 0.1875, ((0, 16), (1, 2))),
        "bubble": jnp.clip(-2.0 + 1.8 * jax.random.uniform(key_list[1], (POINTS, ORDER), jnp.float32) ** block_levels(key_list[1], (POINTS, ORDER), ((0, 16),), -0.2, 0.2), -2.0, -0.2),
        "cross_deriv": gaussian(key_list[2], (POINTS, ORDER, ORDER), 1.0, 6.0, ((0, 16), (1, 2))),
        "send_blocks": draw_send_blocks(jax.random.fold_in(key_list[7], 71), 0),
        "recv_slots": draw_recv_slots(jax.random.fold_in(key_list[7], 71), 0),
        "freq_shift": set_ends(jax.random.randint(key_list[5], (POINTS, NFF), 0 - NFREQ // 4, NFREQ // 4 + 1), jax.random.fold_in(key_list[5], 1), 0 - NFREQ // 4, (NFREQ // 4 + 1) - 1).astype(jnp.int32),
        "proj_coef": jnp.clip(jax.random.uniform(key_list[6], (POINTS, NFF), jnp.float32, -1.5, 1.5) * block_levels(key_list[6], (POINTS, NFF), ((0, 16),), -0.4, 0.0), -1.5, 1.5),
    }


def reference(vertex, bubble, cross_deriv, send_blocks, recv_slots, freq_shift, proj_coef):
    freq_grid = jnp.arange(NFREQ, dtype=jnp.int32)

    def take_box(src_point, src_form, shift_by, weight_of):
        stripe = lax.dynamic_slice(cross_deriv, (src_point, jnp.int32(0), src_form * NFREQ), (1, ORDER, NFREQ))[0]
        source_freq = freq_grid + shift_by
        inside = (source_freq >= 0) & (source_freq < NFREQ)
        shifted = jnp.take(stripe, jnp.clip(source_freq, 0, NFREQ - 1), axis=1)
        return jnp.where(inside[None, :], shifted.astype(jnp.float32) * weight_of, 0.0)

    def one_point(packed):
        point_idx, vertex_pt, bubble_pt, slot_row, shift_row, coef_row = packed
        owner_dev = point_idx // PT_DEV
        source_dev = slot_row // CAP
        block_idx = send_blocks[source_dev, owner_dev, slot_row % CAP]
        src_points = (source_dev * PT_DEV + block_idx // NFF).astype(jnp.int32)
        source_form_list = (block_idx % NFF).astype(jnp.int32)
        box_values = jax.vmap(take_box)(src_points, source_form_list, shift_row, coef_row)
        remapped = box_values.transpose(1, 0, 2).reshape(ORDER, ORDER).astype(jnp.bfloat16)
        scaled = (vertex_pt.astype(jnp.float32) * bubble_pt[None, :]).astype(jnp.bfloat16)
        return jnp.dot(scaled, remapped, preferred_element_type=jnp.float32).astype(jnp.bfloat16)

    return lax.map(one_point, (jnp.arange(POINTS, dtype=jnp.int32), vertex, bubble, recv_slots, freq_shift, proj_coef))
```

```python
import functools

import jax
import jax.numpy as jnp
from jax import lax
from jax.experimental import pallas as pl
from jax.experimental.pallas import tpu as pltpu
from jax.sharding import PartitionSpec as P


LIMIT = 24 * 1024 * 1024


def partner_of(n, me, k):
    return me ^ k if n & (n - 1) == 0 else lax.rem(me + k, n)


def origin_of(n, me, k):
    return me ^ k if n & (n - 1) == 0 else lax.rem(me - k + n, n)


def pack_kernel(n, boxes, width, blocks_ref, cross_ref, *rest):
    slabs, table = rest[:n], rest[n]
    me = lax.axis_index("pts")
    rows = cross_ref.shape[1]
    low = lax.broadcasted_iota(jnp.int32, (rows, 2 * width), 1) < width
    for t in range(boxes // 2):
        tile = cross_ref[0, :, 2 * width * t : 2 * width * (t + 1)]
        turned = jnp.concatenate([tile[:, width:], tile[:, :width]], axis=1)
        table[2 * t] = jnp.where(low, tile, turned)
        table[2 * t + 1] = jnp.where(low, turned, tile)
    if boxes % 2:
        last = cross_ref[0, :, width * (boxes - 1) : width * boxes]
        table[boxes - 1] = jnp.concatenate([last, last], axis=1)
    for k in range(n):
        dest = partner_of(n, me, k)
        first = jnp.clip(blocks_ref[0, 0, dest], 0, boxes - 1)
        second = jnp.clip(blocks_ref[0, 1, dest], 0, boxes - 1)
        slabs[k][...] = jnp.where(low, table[first], table[second])


def consume_kernel(n, boxes, width, group, first, last, *refs):
    fills_ref, shift_ref, coef_ref, mine_ref, other_ref = refs[:5]
    slabs = refs[5 : 5 + 2 * len(group)]
    held = refs[5 + 2 * len(group) :]
    total = held[-1]
    me = lax.axis_index("pts")
    rows = mine_ref.shape[0]
    lane = lax.broadcasted_iota(jnp.int32, (rows, 2 * width), 1)
    if last and not first:
        for t in range((boxes + 1) // 2):
            total[t] = held[0][t]
    for i, k in enumerate(group):
        product = jnp.dot(mine_ref[...], slabs[2 * i][...], preferred_element_type=jnp.float32)
        product += jnp.dot(other_ref[...], slabs[2 * i + 1][...], preferred_element_type=jnp.float32)
        source = origin_of(n, me, k)
        for c in range(2):
            f = fills_ref[2 * source + c]

            @pl.when(f >= 0)
            def _():
                h, t = lax.rem(f, 2), f // 2
                shift = shift_ref[0, f]
                amount = lax.rem(width * h - width * c - shift + 4 * width, 2 * width)
                moved = pltpu.roll(product, amount, 1) * coef_ref[0, f]
                taken = lane - width * h + shift
                value = jnp.where((taken >= 0) & (taken < width), moved, 0.0)
                here = lane // width == h
                total[t] = jnp.where(here, value, total[t].astype(jnp.float32)).astype(total.dtype)

    if last:
        out_ref = held[-2]
        for t in range((boxes + 1) // 2):
            if 2 * t + 1 < boxes:
                out_ref[0, :, 2 * width * t : 2 * width * (t + 1)] = total[t]
            else:
                out_ref[0, :, 2 * width * t : width * boxes] = total[t][:, :width]


def plan(n):
    far = list(range(n - 1, n // 2 - 1, -1))
    near = list(range(1, n // 2))
    sequence = []
    for i, k in enumerate(far):
        sequence.append(k)
        if i >= 1 and i - 1 < len(near):
            sequence.append(near[i - 1])
    groups = [[0] + near[: len(near) // 2], near[len(near) // 2 :]]
    groups += [far[i : i + 2] for i in range(0, len(far) - 2, 2)] + [[far[-2]], [far[-1]]]
    return sequence, groups


def body(n, vertex, bubble, cross_deriv, send_blocks, recv_slots, freq_shift, proj_coef):
    _, rows, order = vertex.shape
    boxes = recv_slots.shape[1]
    width = order // boxes
    side = lax.axis_index("rows")
    power = n & (n - 1) == 0

    def pairs(k):
        return [(i, i ^ k if power else (i + k) % n) for i in range(n)]

    smem = pl.BlockSpec(memory_space=pltpu.SMEM)
    vmem = pl.BlockSpec(memory_space=pltpu.VMEM)
    slabs = pl.pallas_call(
        functools.partial(pack_kernel, n, boxes, width),
        out_shape=[jax.ShapeDtypeStruct((rows, 2 * width), cross_deriv.dtype)] * n,
        in_specs=[smem, vmem],
        out_specs=[vmem] * n,
        scratch_shapes=[pltpu.VMEM((boxes, rows, 2 * width), cross_deriv.dtype)],
        cost_estimate=pl.CostEstimate(flops=2000000, bytes_accessed=3000000, transcendentals=0),
        compiler_params=pltpu.CompilerParams(vmem_limit_bytes=LIMIT),
        name="pack",
    )(send_blocks.transpose(0, 2, 1), cross_deriv)

    scaled = (vertex[0].astype(jnp.float32) * bubble[0][None, :]).astype(jnp.bfloat16)
    mine = jnp.where(side == 0, scaled[:, :rows], scaled[:, rows:])
    other = jnp.where(side == 0, scaled[:, rows:], scaled[:, :rows])
    named = recv_slots[0][None, :] == jnp.arange(2 * n, dtype=jnp.int32)[:, None]
    fills = jnp.max(jnp.where(named, jnp.arange(boxes, dtype=jnp.int32)[None, :], -1), axis=1)

    sequence, groups = plan(n)
    arrived, across = {0: slabs[0]}, {}
    for k in sequence:
        arrived[k] = lax.ppermute(slabs[k], "pts", pairs(k))
    for k in sum(groups, []):
        across[k] = lax.ppermute(arrived[k], "rows", [(0, 1), (1, 0)])

    tiles = jax.ShapeDtypeStruct(((boxes + 1) // 2, rows, 2 * width), jnp.bfloat16)
    total = None
    for i, group in enumerate(groups):
        first, last = i == 0, i == len(groups) - 1
        operands = [fills, freq_shift, proj_coef, mine, other]
        for k in group:
            operands += [arrived[k], across[k]]
        specs = [smem] * 3 + [vmem] * (len(operands) - 3)
        if not first:
            operands.append(total)
            specs.append(vmem)
        total = pl.pallas_call(
            functools.partial(consume_kernel, n, boxes, width, group, first, last),
            out_shape=jax.ShapeDtypeStruct(vertex.shape, jnp.bfloat16) if last else tiles,
            in_specs=specs,
            out_specs=vmem,
            scratch_shapes=[pltpu.VMEM(tiles.shape, tiles.dtype)] if last else [],
            input_output_aliases={} if first or last else {len(operands) - 1: 0},
            cost_estimate=pl.CostEstimate(
                flops=2 * rows * order * 2 * width * len(group), bytes_accessed=3000000, transcendentals=0
            ),
            compiler_params=pltpu.CompilerParams(vmem_limit_bytes=LIMIT),
        )(*operands)
    return total


def solution(mesh):
    in_specs = (
        P("pts", "rows", None),
        P("pts", None),
        P("pts", "rows", None),
        P("pts", None, None),
        P("pts", None),
        P("pts", None),
        P("pts", None),
    )
    out_specs = P("pts", "rows", None)
    n = mesh.shape["pts"]

    def run(*args):
        return body(n, *args)

    return jax.shard_map(run, mesh=mesh, in_specs=in_specs, out_specs=out_specs, check_vma=False)
```
